32 devices in a mesh: gx: 4 (over z), gy: 4 (over y, x), gz: 2 (over core).
Axes of the slice: x: 2, y: 2, z: 4, core: 2. Of those that a mesh axis runs over, the one named last changes fastest.
Arguments:
- particles: float32 [8, 262144], P(None, ('gx', 'gy', 'gz')), may hold values from -0.5 to 0.5
- dest_key: int32 [262144], P(('gx', 'gy', 'gz')), may hold values from 0 to 31, as said below
- cell_a: int32 [262144], P(('gx', 'gy', 'gz')), may hold values from 0 to 255
- cell_b: int32 [262144], P(('gx', 'gy', 'gz')), may hold values from 0 to 127
- velocity: float32 [2, 1024, 1024], P(None, 'gx', ('gy', 'gz')), may hold values from -6 to 6
Outputs:
- binned: float32 [8, 1048576], P(None, ('gx', 'gy', 'gz'))
- binned_cell: int32 [1048576], P(('gx', 'gy', 'gz'))
The draws below stay inside these ranges and needn't reach their ends.
Inputs may be any that keep to these rules, and one draw needn't show every extreme that they name: Of the particles of one device at most 1024 have any one value of dest_key, and one device is named by exactly 1024 particles of every device.
All inputs are finite; a program needn't handle non-finite values.
Results may differ from the reference program's by a relative error of at most 0.0003.
Values sent between devices are 32-bit elements; how exact they have to be, the bound alone decides.
A program may use at most 64 MiB of HBM per device.

```python
import jax
import jax.numpy as jnp
from jax import lax

P_DEV = 8192
TA = 256
TB = 128
OWNERS = 32
CAP = 1024
TOTAL = 262144
NA = 1024
NB = 1024
N_GY = 4
N_GZ = 2


def draw_dest_key(key, part):
    hot_owner = jax.random.randint(jax.random.fold_in(key, 7), (), 0, OWNERS)
    slot_owner = (jnp.arange(OWNERS * CAP, dtype=jnp.int32) // CAP + hot_owner) % OWNERS

    def one_source(source_dev):
        source_key = jax.random.fold_in(key, source_dev)
        others = jax.random.permutation(source_key, OWNERS * CAP - CAP).astype(jnp.int32) + CAP
        chosen = jnp.concatenate([jnp.arange(CAP, dtype=jnp.int32), others[:P_DEV - CAP]])
        shuffle = jax.random.permutation(jax.random.fold_in(source_key, 1), P_DEV)
        return slot_owner[chosen][shuffle]
    return lax.map(one_source, jnp.arange(OWNERS, dtype=jnp.int32)).reshape(-1)


def place_ends(array, stream_key, smallest, top_value):
    longest = array.shape.index(max(array.shape))
    spots = []
    for shift in (0, 1):
        where = [jax.random.randint(jax.random.fold_in(stream_key, axis), (), 0, length) for axis, length in enumerate(array.shape)]
        where[longest] = (where[longest] + shift) % array.shape[longest]
        spots.append(tuple(where))
    return array.at[spots[0]].set(smallest).at[spots[1]].set(top_value)


def level_of(rng, extent, split, low, high):
    def one(dim, shards_of):
        heights = jax.random.uniform(jax.random.fold_in(jax.random.fold_in(rng, 6), dim), (shards_of,), jnp.float32, low / len(split), high / len(split))
        return jnp.repeat(jnp.exp(heights), extent[dim] // shards_of).reshape((-1,) + (1,) * (len(extent) - dim - 1))

    gain = one(*split[0])
    for cut in split[1:]:
        gain = gain * one(*cut)
    return gain


def scatter_about(key, shape, spread, limit, cuts=(), held_as=jnp.bfloat16):
    drawn = spread * jax.random.normal(key, shape, jnp.float32)
    if cuts:
        drawn = drawn * level_of(key, shape, cuts, -0.22, 0.18)
    return jnp.clip(drawn, -limit, limit).astype(held_as)


def setup_inputs(seed: int = 0) -> dict:
    splits = jax.random.split(jax.random.key(seed), 6)
    particles = jnp.clip(jax.random.uniform(splits[0], (8, TOTAL), jnp.float32, -0.5, 0.5) * level_of(splits[0], (8, TOTAL), ((1, 32),), -0.4, 0.0), -0.5, 0.5)
    dest_key = draw_dest_key(jax.random.fold_in(splits[5], 71), 0)
    cell_a = place_ends(jax.random.randint(splits[2], (TOTAL,), 0, TA), jax.random.fold_in(splits[2], 1), 0, TA - 1).astype(jnp.int32)
    cell_b = place_ends(jax.random.randint(splits[3], (TOTAL,), 0, TB), jax.random.fold_in(splits[3], 1), 0, TB - 1).astype(jnp.int32)
    velocity = scatter_about(splits[4], (2, NA, NB), 1.0, 6.0, ((1, 4), (2, 8)), jnp.float32)
    return {"particles": particles, "dest_key": dest_key, "cell_a": cell_a, "cell_b": cell_b, "velocity": velocity}


step_length = 0.5


def quad_weights(frac):
    return (0.5 * frac * (frac - 1.0), 1.0 - frac * frac, 0.5 * frac * (frac + 1.0))


def reference(particles, dest_key, cell_a, cell_b, velocity):
    source_dev = jnp.arange(TOTAL, dtype=jnp.int32) // P_DEV
    bucket_key = source_dev * OWNERS + dest_key
    ordering = jnp.argsort(bucket_key, stable=True).astype(jnp.int32)
    ordered = bucket_key[ordering]
    first_index = jnp.searchsorted(ordered, ordered, side="left").astype(jnp.int32)
    rank_sorted = jnp.arange(TOTAL, dtype=jnp.int32) - first_index
    ranking = jnp.zeros((TOTAL,), jnp.int32).at[ordering].set(rank_sorted)
    slot_index = dest_key * (OWNERS * CAP) + source_dev * CAP + ranking
    tile_columns = N_GY * N_GZ
    global_a = (dest_key // tile_columns) * TA + cell_a
    global_b = (dest_key % tile_columns) * TB + cell_b
    padded = jnp.pad(velocity, ((0, 0), (1, 1), (1, 1)))
    row_stride = NB + 2
    flat_field = padded.reshape(2, -1)
    center = ((global_a + 1) * row_stride + global_b + 1).astype(jnp.int32)
    weights_a = quad_weights(particles[0])
    weights_b = quad_weights(particles[1])
    speed = jnp.zeros((2, TOTAL), jnp.float32)
    for shift_a in range(3):
        for shift_b in range(3):
            nodes = flat_field[:, center + (shift_a - 1) * row_stride + (shift_b - 1)]
            speed = speed + weights_a[shift_a] * weights_b[shift_b] * nodes
    advanced = jnp.concatenate([particles[0:2], particles[2:4] + step_length * speed, particles[4:8]], axis=0)
    binned = jnp.zeros((8, OWNERS * OWNERS * CAP), particles.dtype).at[:, slot_index].set(advanced)
    binned_cell = jnp.full((OWNERS * OWNERS * CAP,), -1, jnp.int32).at[slot_index].set(cell_a * TB + cell_b)
    return binned, binned_cell
```

```python
import functools

import jax
import jax.numpy as jnp
from jax import lax
from jax.experimental import pallas as pl
from jax.experimental.pallas import tpu as pltpu
from jax.sharding import PartitionSpec as P

step_length = 0.5
NT = (((1,), (1,)), ((), ()))


def extended(x, sides, width):
    for axis, dim in sides:
        peers, length = (lax.axis_size(axis), x.shape[dim])
        up = [(i, (i + 1) % peers) for i in range(peers - 1)]
        down = [(j, i) for i, j in up]
        last = lax.slice_in_dim(x, length - width, length, axis=dim)
        initial = lax.slice_in_dim(x, 0, width, axis=dim)
        before = lax.ppermute(last, axis, up)
        after = lax.ppermute(initial, axis, down)
        x = jnp.concatenate([before, x, after], axis=dim)
    return x


def quad_weights(frac):
    return (0.5 * frac * (frac - 1.0), 1.0 - frac * frac, 0.5 * frac * (frac + 1.0))


def rounded(x):
    return x.astype(jnp.bfloat16).astype(jnp.float32)


def bucket_kernel(owners, cap, tile_width, chunk, block, part_ref, key_ref, a_ref, b_ref,
                  out_ref, acc_ref, seen_ref, lhs_ref, hot_ref):
    count = key_ref.shape[1]
    acc_ref[...] = jnp.zeros_like(acc_ref)
    seen_ref[...] = jnp.zeros_like(seen_ref)
    upper = (lax.broadcasted_iota(jnp.int32, (block, block), 0)
             < lax.broadcasted_iota(jnp.int32, (block, block), 1)).astype(jnp.float32).astype(jnp.bfloat16)
    owner_ids = lax.broadcasted_iota(jnp.int32, (owners, block), 0)
    rank_ids = lax.broadcasted_iota(jnp.int32, (cap, block), 0)

    def one_chunk(index, carry):
        for part in range(chunk // block):
            start = pl.multiple_of(index * chunk + part * block, block)
            at = slice(part * block, (part + 1) * block)
            keys = key_ref[:, pl.ds(start, block)]
            is_owner = owner_ids == keys
            hot = is_owner.astype(jnp.float32)
            before = jnp.dot(hot.astype(jnp.bfloat16), upper, preferred_element_type=jnp.float32)
            seen = seen_ref[...]
            ranks = jnp.sum(hot * (before + seen[:, :1]), axis=0, keepdims=True).astype(jnp.int32)
            seen_ref[...] = seen + jnp.sum(hot, axis=1, keepdims=True)
            values = part_ref[:, pl.ds(start, block)]
            high = rounded(values)
            both = jnp.concatenate([high, values - high], axis=0)
            for owner in range(owners):
                lhs_ref[owner * 16:(owner + 1) * 16, at] = jnp.where(
                    keys == owner, both, 0.0).astype(jnp.bfloat16)
            rows = (a_ref[:, pl.ds(start, block)] + 1).astype(jnp.float32)
            cols = b_ref[:, pl.ds(start, block)].astype(jnp.float32)
            lhs_ref[owners * 16:owners * 17, at] = (hot * rows).astype(jnp.bfloat16)
            lhs_ref[owners * 17:owners * 18, at] = (hot * cols).astype(jnp.bfloat16)
            hot_ref[:, at] = (rank_ids == ranks).astype(jnp.float32).astype(jnp.bfloat16)
        acc_ref[...] += lax.dot_general(lhs_ref[...], hot_ref[...], NT,
                                        preferred_element_type=jnp.float32)
        return carry

    lax.fori_loop(0, count // chunk, one_chunk, 0)
    cells = (acc_ref[owners * 16:owners * 17, :] * float(tile_width)
             + acc_ref[owners * 17:owners * 18, :] - float(tile_width))
    for owner in range(owners):
        low = owner * 16
        out_ref[owner, :, :cap] = acc_ref[low:low + 8, :] + acc_ref[low + 8:low + 16, :]
        for j in range(cap // 128):
            out_ref[owner, j:j + 1, cap:] = cells[owner:owner + 1, j * 128:(j + 1) * 128]
        if cap // 128 < 8:
            out_ref[owner, cap // 128:, cap:] = jnp.zeros((8 - cap // 128, 128), jnp.float32)


def banded(index, weights, height):
    diff = lax.broadcasted_iota(jnp.int32, (height, index.shape[1]), 0) - index
    masks = [diff == shift for shift in range(3)]
    return [jnp.where(masks[0], w[0], jnp.where(masks[1], w[1], jnp.where(masks[2], w[2], 0.0)))
            for w in weights]


def advance(block, cap, tile_width, lhs, piece):
    values = block[:, :cap]
    cells = jnp.concatenate([block[j:j + 1, cap:] for j in range(cap // 128)], axis=1)
    cells = cells.astype(jnp.int32)
    rows_out, cells_out = [], []
    width = lhs.shape[0] // 2
    height = lhs.shape[1] // 3
    for start in range(0, cap, piece):
        v = values[:, start:start + piece]
        cell = cells[:, start:start + piece]
        live = cell >= 0
        safe = jnp.maximum(cell, 0)
        node_row = safe // tile_width
        node_col = safe - node_row * tile_width
        wa = quad_weights(v[0:1])
        wb = quad_weights(v[1:2])
        high = [rounded(w) for w in wa]
        low = [w - h for w, h in zip(wa, high)]
        w_high, w_low = banded(node_row, (high, low), height)
        w_high = w_high.astype(jnp.bfloat16)
        w_low = w_low.astype(jnp.bfloat16)
        mixed = jnp.dot(lhs, jnp.concatenate([w_high, w_high, w_low], axis=0),
                        preferred_element_type=jnp.float32)
        (col_weight,) = banded(node_col, (wb,), width)
        scale = jnp.where(live, step_length, 0.0)
        first = jnp.sum(mixed[:width] * col_weight, axis=0, keepdims=True) * scale
        second = jnp.sum(mixed[width:] * col_weight, axis=0, keepdims=True) * scale
        row = lax.broadcasted_iota(jnp.int32, v.shape, 0)
        rows_out.append(v + jnp.where(row == 2, first, jnp.where(row == 3, second, 0.0)))
        cells_out.append(jnp.where(live, cell, -1))
    return rows_out, cells_out


def interp_kernel(cap, tile_width, piece, arrived_ref, lhs_ref, out_ref, cell_ref):
    rows_out, cells_out = advance(arrived_ref[0], cap, tile_width, lhs_ref[...], piece)
    for k, start in enumerate(range(0, cap, piece)):
        out_ref[:, start:start + piece] = rows_out[k]
        cell_ref[:, start:start + piece] = cells_out[k]


def field_matrix(velocity):
    tile_height, tile_width = velocity.shape[1:]
    height = -(-(tile_height + 2) // 16) * 16
    width = -(-(tile_width + 2) // 8) * 8
    padded = extended(velocity, (("gx", 1), (("gy", "gz"), 2)), 1)
    flat = jnp.transpose(padded, (0, 2, 1))
    flat = jnp.pad(flat, ((0, 0), (0, width - tile_width - 2), (0, height - tile_height - 2)))
    flat = flat.reshape(2 * width, height)
    high = lax.reduce_precision(flat, 8, 7)
    low = flat - high
    return jnp.concatenate([high, low, high], axis=1).astype(jnp.bfloat16)


def shards(particles, dest_key, cell_a, cell_b, velocity):
    owners = lax.axis_size(("gx", "gy", "gz"))
    count = particles.shape[1]
    cap = 4 * count // owners
    tile_height, tile_width = velocity.shape[1:]
    assert tile_height <= 256 and tile_width <= 256 and cap % 128 == 0 and cap <= 1024
    chunk, block = 1024, 256
    outgoing = pl.pallas_call(
        functools.partial(bucket_kernel, owners, cap, tile_width, chunk, block),
        out_shape=jax.ShapeDtypeStruct((owners, 8, cap + 128), jnp.float32),
        in_specs=[pl.BlockSpec(memory_space=pltpu.VMEM)] * 4,
        out_specs=pl.BlockSpec(memory_space=pltpu.VMEM),
        scratch_shapes=[
            pltpu.VMEM((owners * 18, cap), jnp.float32),
            pltpu.VMEM((owners, 128), jnp.float32),
            pltpu.VMEM((owners * 18, chunk), jnp.bfloat16),
            pltpu.VMEM((cap, chunk), jnp.bfloat16),
        ],
        cost_estimate=pl.CostEstimate(flops=2 * 18 * owners * cap * count,
                                      bytes_accessed=4 * 12 * count, transcendentals=0),
    )(particles, dest_key.reshape(1, -1), cell_a.reshape(1, -1), cell_b.reshape(1, -1))
    lhs = field_matrix(velocity)
    arrived = lax.all_to_all(outgoing, ("gx", "gy", "gz"), split_axis=0, concat_axis=0, tiled=True)
    piece = min(cap, 256)
    binned, binned_cell = pl.pallas_call(
        functools.partial(interp_kernel, cap, tile_width, piece),
        out_shape=(jax.ShapeDtypeStruct((8, owners * cap), jnp.float32),
                   jax.ShapeDtypeStruct((1, owners * cap), jnp.int32)),
        grid=(owners,),
        in_specs=[pl.BlockSpec((1, 8, cap + 128), lambda i: (i, 0, 0)),
                  pl.BlockSpec(lhs.shape, lambda i: (0, 0))],
        out_specs=(pl.BlockSpec((8, cap), lambda i: (0, i)),
                   pl.BlockSpec((1, cap), lambda i: (0, i))),
    )(arrived, lhs)
    return (binned, binned_cell.reshape(-1))


def solution(mesh):
    in_specs = (
        P(None, ("gx", "gy", "gz")),
        P(("gx", "gy", "gz")),
        P(("gx", "gy", "gz")),
        P(("gx", "gy", "gz")),
        P(None, "gx", ("gy", "gz")),
    )
    out_specs = (P(None, ("gx", "gy", "gz")), P(("gx", "gy", "gz")))
    return jax.shard_map(shards, mesh=mesh, in_specs=in_specs, out_specs=out_specs, check_vma=False)
```

```python
import functools

import jax
import jax.numpy as jnp
from jax import lax
from jax.experimental import pallas as pl
from jax.experimental.pallas import tpu as pltpu
from jax.sharding import PartitionSpec as P

step_length = 0.5
NT = (((1,), (1,)), ((), ()))


def quad_weights(frac):
    return (0.5 * frac * (frac - 1.0), 1.0 - frac * frac, 0.5 * frac * (frac + 1.0))


def rounded(x):
    return x.astype(jnp.bfloat16).astype(jnp.float32)


def bucket_kernel(owners, cap, tile_width, chunk, block, part_ref, key_ref, a_ref, b_ref,
                  out_ref, acc_ref, seen_ref, lhs_ref, hot_ref):
    count = key_ref.shape[1]
    acc_ref[...] = jnp.zeros_like(acc_ref)
    seen_ref[...] = jnp.zeros_like(seen_ref)
    upper = (lax.broadcasted_iota(jnp.int32, (block, block), 0)
             < lax.broadcasted_iota(jnp.int32, (block, block), 1)).astype(jnp.float32).astype(jnp.bfloat16)
    owner_ids = lax.broadcasted_iota(jnp.int32, (owners, block), 0)
    rank_ids = lax.broadcasted_iota(jnp.int32, (cap, block), 0)

    def one_chunk(index, carry):
        for part in range(chunk // block):
            start = pl.multiple_of(index * chunk + part * block, block)
            at = slice(part * block, (part + 1) * block)
            keys = key_ref[:, pl.ds(start, block)]
            is_owner = owner_ids == keys
            hot = is_owner.astype(jnp.float32)
            before = jnp.dot(hot.astype(jnp.bfloat16), upper, preferred_element_type=jnp.float32)
            seen = seen_ref[...]
            ranks = jnp.sum(hot * (before + seen[:, :1]), axis=0, keepdims=True).astype(jnp.int32)
            seen_ref[...] = seen + jnp.sum(hot, axis=1, keepdims=True)
            values = part_ref[:, pl.ds(start, block)]
            high = rounded(values)
            both = jnp.concatenate([high, values - high], axis=0)
            for owner in range(owners):
                lhs_ref[owner * 16:(owner + 1) * 16, at] = jnp.where(
                    keys == owner, both, 0.0).astype(jnp.bfloat16)
            rows = (a_ref[:, pl.ds(start, block)] + 1).astype(jnp.float32)
            cols = b_ref[:, pl.ds(start, block)].astype(jnp.float32)
            lhs_ref[owners * 16:owners * 17, at] = (hot * rows).astype(jnp.bfloat16)
            lhs_ref[owners * 17:owners * 18, at] = (hot * cols).astype(jnp.bfloat16)
            hot_ref[:, at] = (rank_ids == ranks).astype(jnp.float32).astype(jnp.bfloat16)
        acc_ref[...] += lax.dot_general(lhs_ref[...], hot_ref[...], NT,
                                        preferred_element_type=jnp.float32)
        return carry

    lax.fori_loop(0, count // chunk, one_chunk, 0)
    cells = (acc_ref[owners * 16:owners * 17, :] * float(tile_width)
             + acc_ref[owners * 17:owners * 18, :] - float(tile_width))
    for owner in range(owners):
        low = owner * 16
        out_ref[owner, :, :cap] = acc_ref[low:low + 8, :] + acc_ref[low + 8:low + 16, :]
        for j in range(cap // 128):
            out_ref[owner, j:j + 1, cap:] = cells[owner:owner + 1, j * 128:(j + 1) * 128]
        if cap // 128 < 8:
            out_ref[owner, cap // 128:, cap:] = jnp.zeros((8 - cap // 128, 128), jnp.float32)


def banded(node, index, weights):
    diff = node - index
    masks = [diff == shift for shift in (-1, 0, 1)]
    return [jnp.where(masks[0], w[0], jnp.where(masks[1], w[1], jnp.where(masks[2], w[2], 0.0)))
            for w in weights]


def advance(block, cap, tile_height, tile_width, lhs_ref, piece):
    values = block[:, :cap]
    cells = jnp.concatenate([block[j:j + 1, cap:] for j in range(cap // 128)], axis=1)
    cells = cells.astype(jnp.int32)
    rows_out, cells_out = [], []
    width = lhs_ref.shape[0] // 2
    depth = 3 * tile_height + 16
    row_node = lax.broadcasted_iota(jnp.int32, (tile_height, piece), 0)
    col_node = lax.broadcasted_iota(jnp.int32, (width, piece), 0)
    col_node = jnp.where(col_node < tile_width, col_node, jnp.where(
        col_node == tile_width, -1, jnp.where(col_node == tile_width + 1, tile_width, -5)))
    spare = lax.broadcasted_iota(jnp.int32, (16, piece), 0)
    for start in range(0, cap, piece):
        v = values[:, start:start + piece]
        cell = cells[:, start:start + piece]
        live = cell >= 0
        safe = jnp.maximum(cell, 0)
        node_row = safe // tile_width
        node_col = safe - node_row * tile_width
        wa = quad_weights(v[0:1])
        wb = quad_weights(v[1:2])
        high = [rounded(w) for w in wa]
        low = [w - h for w, h in zip(wa, high)]
        w_high, w_low = banded(row_node, node_row, (high, low))
        w_high = w_high.astype(jnp.bfloat16)
        w_low = w_low.astype(jnp.bfloat16)
        above, below = node_row == 0, node_row == tile_height - 1
        edge = jnp.where(
            spare < 4,
            jnp.where(spare % 2 == 0, jnp.where(above, high[0], 0.0), jnp.where(below, high[2], 0.0)),
            jnp.where(spare == 4, jnp.where(above, low[0], 0.0),
                      jnp.where(spare == 5, jnp.where(below, low[2], 0.0), 0.0)))
        mixed = jnp.dot(lhs_ref[:, :depth],
                        jnp.concatenate([w_high, w_high, w_low, edge.astype(jnp.bfloat16)], axis=0),
                        preferred_element_type=jnp.float32)
        (col_weight,) = banded(col_node, node_col, (wb,))
        scale = jnp.where(live, step_length, 0.0)
        first = jnp.sum(mixed[:width] * col_weight, axis=0, keepdims=True) * scale
        second = jnp.sum(mixed[width:] * col_weight, axis=0, keepdims=True) * scale
        row = lax.broadcasted_iota(jnp.int32, v.shape, 0)
        rows_out.append(v + jnp.where(row == 2, first, jnp.where(row == 3, second, 0.0)))
        cells_out.append(jnp.where(live, cell, -1))
    return rows_out, cells_out


DIRS = ((-1, -1), (-1, 0), (-1, 1), (0, -1), (0, 1), (1, -1), (1, 0), (1, 1))


def build_lhs(vel_ref, halo_ref, lhs_ref, tile_height, tile_width):
    width = lhs_ref.shape[0] // 2
    lane = lax.broadcasted_iota(jnp.int32, (1, 128), 1)

    def beside(da, db, row):
        return halo_ref[DIRS.index((da, db)), row:row + 1, :]

    for c in range(2):
        own = jnp.transpose(vel_ref[c])
        left = beside(0, -1, 4 * c + 3)[:, :tile_height]
        right = beside(0, 1, 4 * c + 2)[:, :tile_height]
        rest = jnp.zeros((width - tile_width - 2, tile_height), jnp.float32)
        body = jnp.concatenate([own, left, right, rest], axis=0)
        high = rounded(body)
        low = body - high

        def outer(da, row):
            middle = beside(da, 0, row)[:, :tile_width]
            west = beside(da, -1, row)[:, tile_width - 1:tile_width]
            east = beside(da, 1, row)[:, 0:1]
            return jnp.concatenate(
                [middle, jnp.where(lane == 0, west, jnp.where(lane == 1, east, 0.0))], axis=1)

        ends = jnp.concatenate([outer(-1, 4 * c + 1), outer(1, 4 * c)], axis=0)
        ends_high = rounded(ends)
        extra = jnp.concatenate([ends_high, ends - ends_high, ends_high], axis=0)
        extra = jnp.concatenate([extra, jnp.zeros((122, extra.shape[1]), jnp.float32)], axis=0)
        extra = jnp.transpose(extra)[:width]
        lhs_ref[c * width:(c + 1) * width, :] = jnp.concatenate(
            [high, low, high, extra], axis=1).astype(jnp.bfloat16)


def exchange_kernel(sizes, cap, piece, out_going_ref, edge_ref, vel_ref, out_ref, cell_ref,
                    held, halo_ref, lhs_ref, own_sem, send_sem, recv_sem, halo_send, halo_recv):
    nx, ny, nz = sizes
    plane = ny * nz
    n = nx * plane
    tile_height, tile_width = vel_ref.shape[1:]
    gx, gy, gz = lax.axis_index("gx"), lax.axis_index("gy"), lax.axis_index("gz")
    column = gy * nz + gz

    def at(dx, dyz, sign):
        x = lax.rem(gx + sign * dx + nx, nx)
        y = lax.rem(gy + sign * (dyz // nz) + ny, ny)
        z = lax.rem(gz + sign * lax.rem(dyz, nz) + nz, nz)
        return x, y, z

    def linear(place):
        return (place[0] * ny + place[1]) * nz + place[2]

    def halo_copy(k):
        da, db = DIRS[k]
        there = column + db
        return pltpu.make_async_remote_copy(
            src_ref=edge_ref, dst_ref=halo_ref.at[7 - k], send_sem=halo_send.at[k],
            recv_sem=halo_recv.at[7 - k], device_id=(gx + da, there // nz, lax.rem(there, nz)),
            device_id_type=pl.DeviceIdType.MESH)

    def halo_arrival(k):
        da, db = DIRS[k]
        there = column + db
        return pltpu.make_async_remote_copy(
            src_ref=edge_ref, dst_ref=halo_ref.at[k], send_sem=halo_send.at[k],
            recv_sem=halo_recv.at[k], device_id=(gx + da, there // nz, lax.rem(there, nz)),
            device_id_type=pl.DeviceIdType.MESH)

    def exists(k):
        da, db = DIRS[k]
        a, b = gx + da, column + db
        return (a >= 0) & (a < nx) & (b >= 0) & (b < plane)

    def block_copy(dx, dyz):
        target = at(dx, dyz, 1)
        slot = dx * plane + dyz
        return pltpu.make_async_remote_copy(
            src_ref=out_going_ref.at[linear(target)], dst_ref=held.at[slot],
            send_sem=send_sem.at[slot], recv_sem=recv_sem.at[slot], device_id=target,
            device_id_type=pl.DeviceIdType.MESH)

    for k in range(8):
        @pl.when(exists(k))
        def _(k=k):
            halo_copy(k).start()

        @pl.when(jnp.logical_not(exists(k)))
        def _(k=k):
            halo_ref[k] = jnp.zeros(halo_ref.shape[1:], jnp.float32)

    own = pltpu.make_async_copy(out_going_ref.at[linear((gx, gy, gz))], held.at[0], own_sem)
    own.start()

    def send(q, carry):
        block_copy(lax.rem(q, nx), q // nx).start()
        return carry

    lax.fori_loop(1, n, send, 0)

    for k in range(8):
        @pl.when(exists(k))
        def _(k=k):
            halo_arrival(k).wait_recv()

    build_lhs(vel_ref, halo_ref, lhs_ref, tile_height, tile_width)

    def work(dx, dyz):
        slot = dx * plane + dyz
        source = linear(at(dx, dyz, -1))
        rows_out, cells_out = advance(held[slot], cap, tile_height, tile_width, lhs_ref, piece)
        for k, start in enumerate(range(0, cap, piece)):
            spot = pl.ds(pl.multiple_of(source * cap + start, 128), piece)
            out_ref[:, spot] = rows_out[k]
            cell_ref[:, spot] = cells_out[k]

    own.wait()

    def one(q, carry):
        near = q < plane
        r = jnp.maximum(q - plane, 0)
        dx = jnp.where(near, 0, lax.rem(r, nx - 1) + 1)
        dyz = jnp.where(near, q, r // (nx - 1))

        @pl.when(q > 0)
        def _():
            block_copy(dx, dyz).wait_recv()

        work(dx, dyz)
        return carry

    lax.fori_loop(0, n, one, 0)

    def sent(q, carry):
        block_copy(lax.rem(q, nx), q // nx).wait_send()
        return carry

    lax.fori_loop(1, n, sent, 0)
    for k in range(8):
        @pl.when(exists(k))
        def _(k=k):
            halo_copy(k).wait_send()


def shards(particles, dest_key, cell_a, cell_b, velocity):
    owners = lax.axis_size(("gx", "gy", "gz"))
    count = particles.shape[1]
    cap = 4 * count // owners
    tile_height, tile_width = velocity.shape[1:]
    assert tile_height <= 256 and tile_width <= 256 and cap % 128 == 0 and cap <= 1024
    chunk, block = 1024, 256
    outgoing = pl.pallas_call(
        functools.partial(bucket_kernel, owners, cap, tile_width, chunk, block),
        out_shape=jax.ShapeDtypeStruct((owners, 8, cap + 128), jnp.float32),
        in_specs=[pl.BlockSpec(memory_space=pltpu.VMEM)] * 4,
        out_specs=pl.BlockSpec(memory_space=pltpu.VMEM),
        scratch_shapes=[
            pltpu.VMEM((owners * 18, cap), jnp.float32),
            pltpu.VMEM((owners, 128), jnp.float32),
            pltpu.VMEM((owners * 18, chunk), jnp.bfloat16),
            pltpu.VMEM((cap, chunk), jnp.bfloat16),
        ],
        cost_estimate=pl.CostEstimate(flops=2 * 18 * owners * cap * count,
                                      bytes_accessed=4 * 12 * count, transcendentals=0),
    )(particles, dest_key.reshape(1, -1), cell_a.reshape(1, -1), cell_b.reshape(1, -1))
    reach = max(tile_height, tile_width)
    lines = []
    for c in range(2):
        for line in (velocity[c, 0], velocity[c, -1], velocity[c, :, 0], velocity[c, :, -1]):
            lines.append(jnp.pad(line, (0, reach - line.shape[0])))
    edges = jnp.stack(lines, axis=0)
    piece = min(cap, 256)
    width = -(-(tile_width + 2) // 8) * 8
    sizes = tuple(lax.axis_size(name) for name in ("gx", "gy", "gz"))
    binned, binned_cell = pl.pallas_call(
        functools.partial(exchange_kernel, sizes, cap, piece),
        out_shape=(jax.ShapeDtypeStruct((8, owners * cap), jnp.float32),
                   jax.ShapeDtypeStruct((1, owners * cap), jnp.int32)),
        in_specs=[pl.BlockSpec(memory_space=pl.ANY)] + [pl.BlockSpec(memory_space=pltpu.VMEM)] * 2,
        out_specs=(pl.BlockSpec(memory_space=pltpu.VMEM),) * 2,
        scratch_shapes=[
            pltpu.VMEM((owners, 8, cap + 128), jnp.float32),
            pltpu.VMEM((8, 8, reach), jnp.float32),
            pltpu.VMEM((2 * width, 3 * tile_height + 128), jnp.bfloat16),
            pltpu.SemaphoreType.DMA,
            pltpu.SemaphoreType.DMA((owners,)),
            pltpu.SemaphoreType.DMA((owners,)),
            pltpu.SemaphoreType.DMA((8,)),
            pltpu.SemaphoreType.DMA((8,)),
        ],
        compiler_params=pltpu.CompilerParams(has_side_effects=True),
    )(outgoing, edges, velocity)
    return (binned, binned_cell.reshape(-1))


def solution(mesh):
    in_specs = (
        P(None, ("gx", "gy", "gz")),
        P(("gx", "gy", "gz")),
        P(("gx", "gy", "gz")),
        P(("gx", "gy", "gz")),
        P(None, "gx", ("gy", "gz")),
    )
    out_specs = (P(None, ("gx", "gy", "gz")), P(("gx", "gy", "gz")))
    return jax.shard_map(shards, mesh=mesh, in_specs=in_specs, out_specs=out_specs, check_vma=False)
```

```python
import functools

import jax
import jax.numpy as jnp
from jax import lax
from jax.experimental import pallas as pl
from jax.experimental.pallas import tpu as pltpu
from jax.sharding import PartitionSpec as P

step_length = 0.5
NT = (((1,), (1,)), ((), ()))


def quad_weights(frac):
    return (0.5 * frac * (frac - 1.0), 1.0 - frac * frac, 0.5 * frac * (frac + 1.0))


def rounded(x):
    return x.astype(jnp.bfloat16).astype(jnp.float32)


def bucket_kernel(owners, cap, tile_width, chunk, block, part_ref, key_ref, a_ref, b_ref, vel_ref,
                  out_ref, edge_ref, acc_ref, seen_ref, lhs_ref, hot_ref):
    count = key_ref.shape[1]
    tile_height = vel_ref.shape[1]
    edge_ref[...] = jnp.zeros_like(edge_ref)
    for c in range(2):
        edge_ref[4 * c:4 * c + 1, :tile_width] = vel_ref[c, 0:1, :]
        edge_ref[4 * c + 1:4 * c + 2, :tile_width] = vel_ref[c, tile_height - 1:, :]
        turned = jnp.transpose(vel_ref[c])
        edge_ref[4 * c + 2:4 * c + 3, :tile_height] = turned[0:1]
        edge_ref[4 * c + 3:4 * c + 4, :tile_height] = turned[tile_width - 1:]
    acc_ref[...] = jnp.zeros_like(acc_ref)
    seen_ref[...] = jnp.zeros_like(seen_ref)
    upper = (lax.broadcasted_iota(jnp.int32, (block, block), 0)
             < lax.broadcasted_iota(jnp.int32, (block, block), 1)).astype(jnp.float32).astype(jnp.bfloat16)
    owner_ids = lax.broadcasted_iota(jnp.int32, (owners, block), 0)
    rank_ids = lax.broadcasted_iota(jnp.int32, (cap, block), 0)

    def one_chunk(index, carry):
        for part in range(chunk // block):
            start = pl.multiple_of(index * chunk + part * block, block)
            at = slice(part * block, (part + 1) * block)
            keys = key_ref[:, pl.ds(start, block)]
            is_owner = owner_ids == keys
            hot = is_owner.astype(jnp.float32)
            before = jnp.dot(hot.astype(jnp.bfloat16), upper, preferred_element_type=jnp.float32)
            seen = seen_ref[...]
            ranks = jnp.sum(hot * (before + seen[:, :1]), axis=0, keepdims=True).astype(jnp.int32)
            seen_ref[...] = seen + jnp.sum(hot, axis=1, keepdims=True)
            values = part_ref[:, pl.ds(start, block)]
            high = rounded(values)
            both = jnp.concatenate([high, values - high], axis=0)
            for owner in range(owners):
                lhs_ref[owner * 16:(owner + 1) * 16, at] = jnp.where(
                    keys == owner, both, 0.0).astype(jnp.bfloat16)
            rows = (a_ref[:, pl.ds(start, block)] + 1).astype(jnp.float32)
            cols = b_ref[:, pl.ds(start, block)].astype(jnp.float32)
            lhs_ref[owners * 16:owners * 17, at] = (hot * rows).astype(jnp.bfloat16)
            lhs_ref[owners * 17:owners * 18, at] = (hot * cols).astype(jnp.bfloat16)
            hot_ref[:, at] = (rank_ids == ranks).astype(jnp.float32).astype(jnp.bfloat16)
        acc_ref[...] += lax.dot_general(lhs_ref[...], hot_ref[...], NT,
                                        preferred_element_type=jnp.float32)
        return carry

    lax.fori_loop(0, count // chunk, one_chunk, 0)
    cells = (acc_ref[owners * 16:owners * 17, :] * float(tile_width)
             + acc_ref[owners * 17:owners * 18, :] - float(tile_width))
    for owner in range(owners):
        low = owner * 16
        out_ref[owner, :, :cap] = acc_ref[low:low + 8, :] + acc_ref[low + 8:low + 16, :]
        for j in range(cap // 128):
            out_ref[owner, j:j + 1, cap:] = cells[owner:owner + 1, j * 128:(j + 1) * 128]
        if cap // 128 < 8:
            out_ref[owner, cap // 128:, cap:] = jnp.zeros((8 - cap // 128, 128), jnp.float32)


def banded(node, index, weights):
    diff = node - index
    masks = [diff == shift for shift in (-1, 0, 1)]
    return [jnp.where(masks[0], w[0], jnp.where(masks[1], w[1], jnp.where(masks[2], w[2], jnp.zeros_like(w[2]))))
            for w in weights]


def advance(block, cap, tile_height, tile_width, lhs_ref, piece):
    values = block[:, :cap]
    cells = jnp.concatenate([block[j:j + 1, cap:] for j in range(cap // 128)], axis=1)
    cells = cells.astype(jnp.int32)
    rows_out, cells_out = [], []
    width = lhs_ref.shape[0] // 2
    depth = 3 * tile_height + 16
    row_node = lax.broadcasted_iota(jnp.int32, (tile_height, piece), 0).astype(jnp.float32).astype(jnp.bfloat16)
    col_node = lax.broadcasted_iota(jnp.int32, (width, piece), 0)
    col_node = jnp.where(col_node < tile_width, col_node, jnp.where(
        col_node == tile_width, -1, jnp.where(col_node == tile_width + 1, tile_width, -5)))
    spare = lax.broadcasted_iota(jnp.int32, (16, piece), 0)
    for start in range(0, cap, piece):
        v = values[:, start:start + piece]
        cell = cells[:, start:start + piece]
        live = cell >= 0
        safe = jnp.maximum(cell, 0)
        node_row = safe // tile_width
        node_col = safe - node_row * tile_width
        wa = quad_weights(v[0:1])
        wb = quad_weights(v[1:2])
        high = [rounded(w) for w in wa]
        low = [w - h for w, h in zip(wa, high)]
        narrow = [[w.astype(jnp.bfloat16) for w in ws] for ws in (high, low)]
        w_high, w_low = banded(row_node, node_row.astype(jnp.float32).astype(jnp.bfloat16), narrow)
        above, below = node_row == 0, node_row == tile_height - 1
        edge = jnp.where(
            spare < 4,
            jnp.where(spare % 2 == 0, jnp.where(above, high[0], 0.0), jnp.where(below, high[2], 0.0)),
            jnp.where(spare == 4, jnp.where(above, low[0], 0.0),
                      jnp.where(spare == 5, jnp.where(below, low[2], 0.0), 0.0)))
        mixed = jnp.dot(lhs_ref[:, :depth],
                        jnp.concatenate([w_high, w_high, w_low, edge.astype(jnp.bfloat16)], axis=0),
                        preferred_element_type=jnp.float32)
        (col_weight,) = banded(col_node, node_col, (wb,))
        scale = jnp.where(live, step_length, 0.0)
        first = jnp.sum(mixed[:width] * col_weight, axis=0, keepdims=True) * scale
        second = jnp.sum(mixed[width:] * col_weight, axis=0, keepdims=True) * scale
        row = lax.broadcasted_iota(jnp.int32, v.shape, 0)
        rows_out.append(v + jnp.where(row == 2, first, jnp.where(row == 3, second, 0.0)))
        cells_out.append(jnp.where(live, cell, -1))
    return rows_out, cells_out


DIRS = ((-1, -1), (-1, 0), (-1, 1), (0, -1), (0, 1), (1, -1), (1, 0), (1, 1))


def build_lhs(vel_ref, halo_ref, lhs_ref, tile_height, tile_width):
    width = lhs_ref.shape[0] // 2
    lane = lax.broadcasted_iota(jnp.int32, (1, 128), 1)

    def beside(da, db, row):
        return halo_ref[DIRS.index((da, db)), row:row + 1, :]

    for c in range(2):
        own = jnp.transpose(vel_ref[c])
        left = beside(0, -1, 4 * c + 3)[:, :tile_height]
        right = beside(0, 1, 4 * c + 2)[:, :tile_height]
        rest = jnp.zeros((width - tile_width - 2, tile_height), jnp.float32)
        body = jnp.concatenate([own, left, right, rest], axis=0)
        high = rounded(body)
        low = body - high

        def outer(da, row):
            middle = beside(da, 0, row)[:, :tile_width]
            west = beside(da, -1, row)[:, tile_width - 1:tile_width]
            east = beside(da, 1, row)[:, 0:1]
            return jnp.concatenate(
                [middle, jnp.where(lane == 0, west, jnp.where(lane == 1, east, 0.0))], axis=1)

        ends = jnp.concatenate([outer(-1, 4 * c + 1), outer(1, 4 * c)], axis=0)
        ends_high = rounded(ends)
        extra = jnp.concatenate([ends_high, ends - ends_high, ends_high], axis=0)
        extra = jnp.concatenate([extra, jnp.zeros((122, extra.shape[1]), jnp.float32)], axis=0)
        extra = jnp.transpose(extra)[:width]
        lhs_ref[c * width:(c + 1) * width, :] = jnp.concatenate(
            [high, low, high, extra], axis=1).astype(jnp.bfloat16)


def exchange_kernel(sizes, cap, piece, out_going_ref, edge_ref, vel_ref, out_ref, cell_ref,
                    held, halo_ref, lhs_ref, own_sem, send_sem, recv_sem, halo_send, halo_recv):
    nx, ny, nz = sizes
    plane = ny * nz
    n = nx * plane
    tile_height, tile_width = vel_ref.shape[1:]
    gx, gy, gz = lax.axis_index("gx"), lax.axis_index("gy"), lax.axis_index("gz")
    column = gy * nz + gz

    def at(dx, dyz, sign):
        x = lax.rem(gx + sign * dx + nx, nx)
        y = lax.rem(gy + sign * (dyz // nz) + ny, ny)
        z = lax.rem(gz + sign * lax.rem(dyz, nz) + nz, nz)
        return x, y, z

    def linear(place):
        return (place[0] * ny + place[1]) * nz + place[2]

    def halo_copy(k):
        da, db = DIRS[k]
        there = column + db
        return pltpu.make_async_remote_copy(
            src_ref=edge_ref, dst_ref=halo_ref.at[7 - k], send_sem=halo_send.at[k],
            recv_sem=halo_recv.at[7 - k], device_id=(gx + da, there // nz, lax.rem(there, nz)),
            device_id_type=pl.DeviceIdType.MESH)

    def halo_arrival(k):
        da, db = DIRS[k]
        there = column + db
        return pltpu.make_async_remote_copy(
            src_ref=edge_ref, dst_ref=halo_ref.at[k], send_sem=halo_send.at[k],
            recv_sem=halo_recv.at[k], device_id=(gx + da, there // nz, lax.rem(there, nz)),
            device_id_type=pl.DeviceIdType.MESH)

    def exists(k):
        da, db = DIRS[k]
        a, b = gx + da, column + db
        return (a >= 0) & (a < nx) & (b >= 0) & (b < plane)

    def block_copy(dx, dyz):
        target = at(dx, dyz, 1)
        slot = dx * plane + dyz
        return pltpu.make_async_remote_copy(
            src_ref=out_going_ref.at[linear(target)], dst_ref=held.at[slot],
            send_sem=send_sem.at[slot], recv_sem=recv_sem.at[slot], device_id=target,
            device_id_type=pl.DeviceIdType.MESH)

    for k in range(8):
        @pl.when(exists(k))
        def _(k=k):
            halo_copy(k).start()

        @pl.when(jnp.logical_not(exists(k)))
        def _(k=k):
            halo_ref[k] = jnp.zeros(halo_ref.shape[1:], jnp.float32)

    own = pltpu.make_async_copy(out_going_ref.at[linear((gx, gy, gz))], held.at[0], own_sem)
    own.start()

    def send(q, carry):
        block_copy(lax.rem(q, nx), q // nx).start()
        return carry

    lax.fori_loop(1, n, send, 0)

    for k in range(8):
        @pl.when(exists(k))
        def _(k=k):
            halo_arrival(k).wait_recv()

    build_lhs(vel_ref, halo_ref, lhs_ref, tile_height, tile_width)

    def work(dx, dyz):
        slot = dx * plane + dyz
        source = linear(at(dx, dyz, -1))
        rows_out, cells_out = advance(held[slot], cap, tile_height, tile_width, lhs_ref, piece)
        for k, start in enumerate(range(0, cap, piece)):
            spot = pl.ds(pl.multiple_of(source * cap + start, 128), piece)
            out_ref[:, spot] = rows_out[k]
            cell_ref[:, spot] = cells_out[k]

    own.wait()

    def one(q, carry):
        near = q < plane
        r = jnp.maximum(q - plane, 0)
        dx = jnp.where(near, 0, lax.rem(r, nx - 1) + 1)
        dyz = jnp.where(near, q, r // (nx - 1))

        @pl.when(q > 0)
        def _():
            block_copy(dx, dyz).wait_recv()

        work(dx, dyz)
        return carry

    lax.fori_loop(0, n, one, 0)

    def sent(q, carry):
        block_copy(lax.rem(q, nx), q // nx).wait_send()
        return carry

    lax.fori_loop(1, n, sent, 0)
    for k in range(8):
        @pl.when(exists(k))
        def _(k=k):
            halo_copy(k).wait_send()


def shards(particles, dest_key, cell_a, cell_b, velocity):
    owners = lax.axis_size(("gx", "gy", "gz"))
    count = particles.shape[1]
    cap = 4 * count // owners
    tile_height, tile_width = velocity.shape[1:]
    assert tile_height <= 256 and tile_width <= 256 and cap % 128 == 0 and cap <= 1024
    chunk, block = 1024, 256
    reach = max(tile_height, tile_width)
    outgoing, edges = pl.pallas_call(
        functools.partial(bucket_kernel, owners, cap, tile_width, chunk, block),
        out_shape=(jax.ShapeDtypeStruct((owners, 8, cap + 128), jnp.float32),
                   jax.ShapeDtypeStruct((8, reach), jnp.float32)),
        in_specs=[pl.BlockSpec(memory_space=pltpu.VMEM)] * 5,
        out_specs=(pl.BlockSpec(memory_space=pltpu.VMEM),) * 2,
        scratch_shapes=[
            pltpu.VMEM((owners * 18, cap), jnp.float32),
            pltpu.VMEM((owners, 128), jnp.float32),
            pltpu.VMEM((owners * 18, chunk), jnp.bfloat16),
            pltpu.VMEM((cap, chunk), jnp.bfloat16),
        ],
        cost_estimate=pl.CostEstimate(flops=2 * 18 * owners * cap * count,
                                      bytes_accessed=4 * 12 * count, transcendentals=0),
    )(particles, dest_key.reshape(1, -1), cell_a.reshape(1, -1), cell_b.reshape(1, -1), velocity)
    piece = min(cap, 256)
    width = -(-(tile_width + 2) // 8) * 8
    sizes = tuple(lax.axis_size(name) for name in ("gx", "gy", "gz"))
    binned, binned_cell = pl.pallas_call(
        functools.partial(exchange_kernel, sizes, cap, piece),
        out_shape=(jax.ShapeDtypeStruct((8, owners * cap), jnp.float32),
                   jax.ShapeDtypeStruct((1, owners * cap), jnp.int32)),
        in_specs=[pl.BlockSpec(memory_space=pl.ANY)] + [pl.BlockSpec(memory_space=pltpu.VMEM)] * 2,
        out_specs=(pl.BlockSpec(memory_space=pltpu.VMEM),) * 2,
        scratch_shapes=[
            pltpu.VMEM((owners, 8, cap + 128), jnp.float32),
            pltpu.VMEM((8, 8, reach), jnp.float32),
            pltpu.VMEM((2 * width, 3 * tile_height + 128), jnp.bfloat16),
            pltpu.SemaphoreType.DMA,
            pltpu.SemaphoreType.DMA((owners,)),
            pltpu.SemaphoreType.DMA((owners,)),
            pltpu.SemaphoreType.DMA((8,)),
            pltpu.SemaphoreType.DMA((8,)),
        ],
        compiler_params=pltpu.CompilerParams(has_side_effects=True),
    )(outgoing, edges, velocity)
    return (binned, binned_cell.reshape(-1))


def solution(mesh):
    in_specs = (
        P(None, ("gx", "gy", "gz")),
        P(("gx", "gy", "gz")),
        P(("gx", "gy", "gz")),
        P(("gx", "gy", "gz")),
        P(None, "gx", ("gy", "gz")),
    )
    out_specs = (P(None, ("gx", "gy", "gz")), P(("gx", "gy", "gz")))
    return jax.shard_map(shards, mesh=mesh, in_specs=in_specs, out_specs=out_specs, check_vma=False)
```

```python
import functools

import jax
import jax.numpy as jnp
from jax import lax
from jax.experimental import pallas as pl
from jax.experimental.pallas import tpu as pltpu
from jax.sharding import PartitionSpec as P

step_length = 0.5
NT = (((1,), (1,)), ((), ()))


def quad_weights(frac):
    return (0.5 * frac * (frac - 1.0), 1.0 - frac * frac, 0.5 * frac * (frac + 1.0))


def rounded(x):
    return x.astype(jnp.bfloat16).astype(jnp.float32)


def pack_edges(vel_ref, edge_ref):
    tile_height, tile_width = vel_ref.shape[1:]
    edge_ref[...] = jnp.zeros_like(edge_ref)
    for c in range(2):
        edge_ref[4 * c:4 * c + 1, :tile_width] = vel_ref[c, 0:1, :]
        edge_ref[4 * c + 1:4 * c + 2, :tile_width] = vel_ref[c, tile_height - 1:, :]
        turned = jnp.transpose(vel_ref[c])
        edge_ref[4 * c + 2:4 * c + 3, :tile_height] = turned[0:1]
        edge_ref[4 * c + 3:4 * c + 4, :tile_height] = turned[tile_width - 1:]


def rank_particles(owners, cap, chunk, block, key_ref, seen_ref, hot_ref):
    count = key_ref.shape[1]
    seen_ref[...] = jnp.zeros_like(seen_ref)
    upper = (lax.broadcasted_iota(jnp.int32, (block, block), 0)
             < lax.broadcasted_iota(jnp.int32, (block, block), 1)).astype(jnp.float32).astype(jnp.bfloat16)
    owner_ids = lax.broadcasted_iota(jnp.int32, (owners, block), 0)
    rank_ids = lax.broadcasted_iota(jnp.int32, (cap, block), 0)

    def one_chunk(index, carry):
        for part in range(chunk // block):
            start = pl.multiple_of(index * chunk + part * block, block)
            keys = key_ref[:, pl.ds(start, block)]
            hot = (owner_ids == keys).astype(jnp.float32)
            before = jnp.dot(hot.astype(jnp.bfloat16), upper, preferred_element_type=jnp.float32)
            seen = seen_ref[...]
            ranks = jnp.sum(hot * (before + seen[:, :1]), axis=0, keepdims=True).astype(jnp.int32)
            seen_ref[...] = seen + jnp.sum(hot, axis=1, keepdims=True)
            hot_ref[:, pl.ds(start, block)] = (rank_ids == ranks).astype(jnp.float32).astype(jnp.bfloat16)
        return carry

    lax.fori_loop(0, count // chunk, one_chunk, 0)


def place_group(ids, cap, tile_width, chunk, block, part_ref, key_ref, a_ref, b_ref,
                hot_ref, pick_ref, acc_ref, outs):
    count = key_ref.shape[1]
    group = len(ids)
    acc_ref[...] = jnp.zeros_like(acc_ref)
    row = lax.broadcasted_iota(jnp.int32, (group, block), 0)
    wanted = jnp.zeros((group, block), jnp.int32)
    for i, owner in enumerate(ids):
        wanted = jnp.where(row == i, owner, wanted)

    def one_chunk(index, carry):
        for part in range(chunk // block):
            start = pl.multiple_of(index * chunk + part * block, block)
            at = slice(part * block, (part + 1) * block)
            keys = key_ref[:, pl.ds(start, block)]
            values = part_ref[:, pl.ds(start, block)]
            high = rounded(values)
            both = jnp.concatenate([high, values - high], axis=0)
            for i, owner in enumerate(ids):
                pick_ref[i * 16:(i + 1) * 16, at] = jnp.where(
                    keys == owner, both, 0.0).astype(jnp.bfloat16)
            hot = wanted == keys
            rows = (a_ref[:, pl.ds(start, block)] + 1).astype(jnp.float32)
            cols = b_ref[:, pl.ds(start, block)].astype(jnp.float32)
            pick_ref[group * 16:group * 17, at] = jnp.where(hot, rows, 0.0).astype(jnp.bfloat16)
            pick_ref[group * 17:group * 18, at] = jnp.where(hot, cols, 0.0).astype(jnp.bfloat16)
        columns = pl.ds(pl.multiple_of(index * chunk, chunk), chunk)
        acc_ref[...] += lax.dot_general(pick_ref[...], hot_ref[:, columns], NT,
                                        preferred_element_type=jnp.float32)
        return carry

    lax.fori_loop(0, count // chunk, one_chunk, 0)
    cells = (acc_ref[group * 16:group * 17, :] * float(tile_width)
             + acc_ref[group * 17:group * 18, :] - float(tile_width))
    for i, out in enumerate(outs):
        low = i * 16
        out[:, :cap] = acc_ref[low:low + 8, :] + acc_ref[low + 8:low + 16, :]
        for j in range(cap // 128):
            out[j:j + 1, cap:] = cells[i:i + 1, j * 128:(j + 1) * 128]
        if cap // 128 < 8:
            out[cap // 128:, cap:] = jnp.zeros((8 - cap // 128, 128), jnp.float32)


def banded(node, index, weights):
    diff = node - index
    masks = [diff == shift for shift in (-1, 0, 1)]
    return [jnp.where(masks[0], w[0], jnp.where(masks[1], w[1], jnp.where(masks[2], w[2], jnp.zeros_like(w[2]))))
            for w in weights]


def advance(block, cap, tile_height, tile_width, lhs_ref, piece):
    values = block[:, :cap]
    cells = jnp.concatenate([block[j:j + 1, cap:] for j in range(cap // 128)], axis=1)
    cells = cells.astype(jnp.int32)
    rows_out, cells_out = [], []
    width = lhs_ref.shape[0] // 2
    depth = 3 * tile_height + 16
    row_node = lax.broadcasted_iota(jnp.int32, (tile_height, piece), 0).astype(jnp.float32).astype(jnp.bfloat16)
    col_node = lax.broadcasted_iota(jnp.int32, (width, piece), 0)
    col_node = jnp.where(col_node < tile_width, col_node, jnp.where(
        col_node == tile_width, -1, jnp.where(col_node == tile_width + 1, tile_width, -5)))
    spare = lax.broadcasted_iota(jnp.int32, (16, piece), 0)
    for start in range(0, cap, piece):
        v = values[:, start:start + piece]
        cell = cells[:, start:start + piece]
        live = cell >= 0
        safe = jnp.maximum(cell, 0)
        node_row = safe // tile_width
        node_col = safe - node_row * tile_width
        wa = quad_weights(v[0:1])
        wb = quad_weights(v[1:2])
        high = [rounded(w) for w in wa]
        low = [w - h for w, h in zip(wa, high)]
        narrow = [[w.astype(jnp.bfloat16) for w in ws] for ws in (high, low)]
        w_high, w_low = banded(row_node, node_row.astype(jnp.float32).astype(jnp.bfloat16), narrow)
        above, below = node_row == 0, node_row == tile_height - 1
        edge = jnp.where(
            spare < 4,
            jnp.where(spare % 2 == 0, jnp.where(above, high[0], 0.0), jnp.where(below, high[2], 0.0)),
            jnp.where(spare == 4, jnp.where(above, low[0], 0.0),
                      jnp.where(spare == 5, jnp.where(below, low[2], 0.0), 0.0)))
        mixed = jnp.dot(lhs_ref[:, :depth],
                        jnp.concatenate([w_high, w_high, w_low, edge.astype(jnp.bfloat16)], axis=0),
                        preferred_element_type=jnp.float32)
        (col_weight,) = banded(col_node, node_col, (wb,))
        scale = jnp.where(live, step_length, 0.0)
        first = jnp.sum(mixed[:width] * col_weight, axis=0, keepdims=True) * scale
        second = jnp.sum(mixed[width:] * col_weight, axis=0, keepdims=True) * scale
        row = lax.broadcasted_iota(jnp.int32, v.shape, 0)
        rows_out.append(v + jnp.where(row == 2, first, jnp.where(row == 3, second, 0.0)))
        cells_out.append(jnp.where(live, cell, -1))
    return rows_out, cells_out


DIRS = ((-1, -1), (-1, 0), (-1, 1), (0, -1), (0, 1), (1, -1), (1, 0), (1, 1))


def build_lhs(vel_ref, halo_ref, lhs_ref, tile_height, tile_width):
    width = lhs_ref.shape[0] // 2
    lane = lax.broadcasted_iota(jnp.int32, (1, 128), 1)

    def beside(da, db, row):
        return halo_ref[DIRS.index((da, db)), row:row + 1, :]

    for c in range(2):
        own = jnp.transpose(vel_ref[c])
        left = beside(0, -1, 4 * c + 3)[:, :tile_height]
        right = beside(0, 1, 4 * c + 2)[:, :tile_height]
        rest = jnp.zeros((width - tile_width - 2, tile_height), jnp.float32)
        body = jnp.concatenate([own, left, right, rest], axis=0)
        high = rounded(body)
        low = body - high

        def outer(da, row):
            middle = beside(da, 0, row)[:, :tile_width]
            west = beside(da, -1, row)[:, tile_width - 1:tile_width]
            east = beside(da, 1, row)[:, 0:1]
            return jnp.concatenate(
                [middle, jnp.where(lane == 0, west, jnp.where(lane == 1, east, 0.0))], axis=1)

        ends = jnp.concatenate([outer(-1, 4 * c + 1), outer(1, 4 * c)], axis=0)
        ends_high = rounded(ends)
        extra = jnp.concatenate([ends_high, ends - ends_high, ends_high], axis=0)
        extra = jnp.concatenate([extra, jnp.zeros((122, extra.shape[1]), jnp.float32)], axis=0)
        extra = jnp.transpose(extra)[:width]
        lhs_ref[c * width:(c + 1) * width, :] = jnp.concatenate(
            [high, low, high, extra], axis=1).astype(jnp.bfloat16)


def exchange_kernel(sizes, cap, piece, groups, chunk, block, part_ref, key_ref, a_ref, b_ref, vel_ref,
                    out_ref, cell_ref, outgoing, edge_ref, seen_ref, hot_ref, pick_ref, acc_ref,
                    held, halo_ref, lhs_ref, send_sem, recv_sem, halo_send, halo_recv):
    nx, ny, nz = sizes
    plane = ny * nz
    n = nx * plane
    tile_height, tile_width = vel_ref.shape[1:]
    gx, gy, gz = lax.axis_index("gx"), lax.axis_index("gy"), lax.axis_index("gz")
    column = gy * nz + gz

    def at(dx, dyz, sign):
        x = lax.rem(gx + sign * dx + nx, nx)
        y = lax.rem(gy + sign * (dyz // nz) + ny, ny)
        z = lax.rem(gz + sign * lax.rem(dyz, nz) + nz, nz)
        return x, y, z

    def linear(place):
        return (place[0] * ny + place[1]) * nz + place[2]

    def halo_copy(k):
        da, db = DIRS[k]
        there = column + db
        return pltpu.make_async_remote_copy(
            src_ref=edge_ref, dst_ref=halo_ref.at[7 - k], send_sem=halo_send.at[k],
            recv_sem=halo_recv.at[7 - k], device_id=(gx + da, there // nz, lax.rem(there, nz)),
            device_id_type=pl.DeviceIdType.MESH)

    def halo_arrival(k):
        da, db = DIRS[k]
        there = column + db
        return pltpu.make_async_remote_copy(
            src_ref=edge_ref, dst_ref=halo_ref.at[k], send_sem=halo_send.at[k],
            recv_sem=halo_recv.at[k], device_id=(gx + da, there // nz, lax.rem(there, nz)),
            device_id_type=pl.DeviceIdType.MESH)

    def exists(k):
        da, db = DIRS[k]
        a, b = gx + da, column + db
        return (a >= 0) & (a < nx) & (b >= 0) & (b < plane)

    def block_copy(dx, dyz):
        target = at(dx, dyz, 1)
        slot = dx * plane + dyz
        return pltpu.make_async_remote_copy(
            src_ref=outgoing.at[slot], dst_ref=held.at[slot],
            send_sem=send_sem.at[slot], recv_sem=recv_sem.at[slot], device_id=target,
            device_id_type=pl.DeviceIdType.MESH)

    pack_edges(vel_ref, edge_ref)
    rank_particles(n, cap, chunk, block, key_ref, seen_ref, hot_ref)
    for k in range(8):
        @pl.when(exists(k))
        def _(k=k):
            halo_copy(k).start()

        @pl.when(jnp.logical_not(exists(k)))
        def _(k=k):
            halo_ref[k] = jnp.zeros(halo_ref.shape[1:], jnp.float32)

    share = n // groups
    for g in range(groups):
        ids, outs = [], []
        for q in range(g * share, (g + 1) * share):
            dx, dyz = q % nx, q // nx
            ids.append(linear(at(dx, dyz, 1)))
            outs.append(held.at[0] if q == 0 else outgoing.at[dx * plane + dyz])
        place_group(ids, cap, tile_width, chunk, block, part_ref, key_ref, a_ref, b_ref,
                    hot_ref, pick_ref, acc_ref, outs)
        for q in range(max(1, g * share), (g + 1) * share):
            block_copy(q % nx, q // nx).start()

    for k in range(8):
        @pl.when(exists(k))
        def _(k=k):
            halo_arrival(k).wait_recv()

    build_lhs(vel_ref, halo_ref, lhs_ref, tile_height, tile_width)

    def work(dx, dyz):
        slot = dx * plane + dyz
        source = linear(at(dx, dyz, -1))
        rows_out, cells_out = advance(held[slot], cap, tile_height, tile_width, lhs_ref, piece)
        for k, start in enumerate(range(0, cap, piece)):
            spot = pl.ds(pl.multiple_of(source * cap + start, 128), piece)
            out_ref[:, spot] = rows_out[k]
            cell_ref[:, spot] = cells_out[k]

    def one(q, carry):
        near = q < plane
        r = jnp.maximum(q - plane, 0)
        dx = jnp.where(near, 0, lax.rem(r, nx - 1) + 1)
        dyz = jnp.where(near, q, r // (nx - 1))

        @pl.when(q > 0)
        def _():
            block_copy(dx, dyz).wait_recv()

        work(dx, dyz)
        return carry

    lax.fori_loop(0, n, one, 0)

    def sent(q, carry):
        block_copy(lax.rem(q, nx), q // nx).wait_send()
        return carry

    lax.fori_loop(1, n, sent, 0)
    for k in range(8):
        @pl.when(exists(k))
        def _(k=k):
            halo_copy(k).wait_send()


def shards(particles, dest_key, cell_a, cell_b, velocity):
    owners = lax.axis_size(("gx", "gy", "gz"))
    count = particles.shape[1]
    cap = 4 * count // owners
    tile_height, tile_width = velocity.shape[1:]
    assert tile_height <= 256 and tile_width <= 256 and cap % 128 == 0 and cap <= 1024
    chunk, block, groups = 1024, 256, 2
    reach = max(tile_height, tile_width)
    piece = min(cap, 256)
    width = -(-(tile_width + 2) // 8) * 8
    sizes = tuple(lax.axis_size(name) for name in ("gx", "gy", "gz"))
    picks = owners // groups * 18
    binned, binned_cell = pl.pallas_call(
        functools.partial(exchange_kernel, sizes, cap, piece, groups, chunk, block),
        out_shape=(jax.ShapeDtypeStruct((8, owners * cap), jnp.float32),
                   jax.ShapeDtypeStruct((1, owners * cap), jnp.int32)),
        in_specs=[pl.BlockSpec(memory_space=pltpu.VMEM)] * 5,
        out_specs=(pl.BlockSpec(memory_space=pltpu.VMEM),) * 2,
        scratch_shapes=[
            pltpu.VMEM((owners, 8, cap + 128), jnp.float32),
            pltpu.VMEM((8, reach), jnp.float32),
            pltpu.VMEM((owners, 128), jnp.float32),
            pltpu.VMEM((cap, count), jnp.bfloat16),
            pltpu.VMEM((picks, chunk), jnp.bfloat16),
            pltpu.VMEM((picks, cap), jnp.float32),
            pltpu.VMEM((owners, 8, cap + 128), jnp.float32),
            pltpu.VMEM((8, 8, reach), jnp.float32),
            pltpu.VMEM((2 * width, 3 * tile_height + 128), jnp.bfloat16),
            pltpu.SemaphoreType.DMA((owners,)),
            pltpu.SemaphoreType.DMA((owners,)),
            pltpu.SemaphoreType.DMA((8,)),
            pltpu.SemaphoreType.DMA((8,)),
        ],
        compiler_params=pltpu.CompilerParams(has_side_effects=True),
    )(particles, dest_key.reshape(1, -1), cell_a.reshape(1, -1), cell_b.reshape(1, -1), velocity)
    return (binned, binned_cell.reshape(-1))


def solution(mesh):
    in_specs = (
        P(None, ("gx", "gy", "gz")),
        P(("gx", "gy", "gz")),
        P(("gx", "gy", "gz")),
        P(("gx", "gy", "gz")),
        P(None, "gx", ("gy", "gz")),
    )
    out_specs = (P(None, ("gx", "gy", "gz")), P(("gx", "gy", "gz")))
    return jax.shard_map(shards, mesh=mesh, in_specs=in_specs, out_specs=out_specs, check_vma=False)
```
